32 devices in a mesh: cell: 4 (over y, x), rays: 8 (over z, core).
Axes of the slice: x: 2, y: 2, z: 4, core: 2. Of those that a mesh axis runs over, the one named last changes fastest.
Arguments:
- encodings: float32 [2048, 64, 256], P('rays', 'cell'), may hold values from -6 to 6
- spacing: float32 [2048, 64], P('rays', 'cell'), may hold values from 0.01 to 0.06
- counts: int32 [2048, 4], P('rays', 'cell'), may hold values from 1 to 16
- cell_weights: float32 [4, 4, 256, 256], P('cell'), may hold values from -0.375 to 0.375
- density_head: float32 [4, 256], P('cell'), may hold values from -0.75 to 0.75
- decoder_in: float32 [256, 256], replicated, may hold values from -0.75 to 0.75
- decoder_out: float32 [256, 3], replicated, may hold values from -0.375 to 0.375
- color_grad: float32 [2048, 3], P('rays'), may hold values from -0.75 to 0.75
Outputs:
- layer_grads: float32 [4, 4, 256, 256], P('cell')
- head_grads: float32 [4, 256], P('cell')
- decoder_in_grad: float32 [256, 256], replicated
- decoder_out_grad: float32 [256, 3], replicated
- sample_grad: float32 [2048, 64, 256], P('rays', 'cell')
The draws below stay inside these ranges and needn't reach their ends.
Inputs may be any that keep to these rules, and one draw needn't show every extreme that they name: `counts`: live samples of a ray in a cell occupy the first slots of that cell.
All inputs are finite; a program needn't handle non-finite values.
Results may differ from the reference program's by a relative error of at most 0.0003.
Values sent between devices are 32-bit elements; how exact they have to be, the bound alone decides.
No kernel may reach another device: no remote copies, remote signals or barrier semaphores. Data moves between devices by JAX's collectives and lax.ppermute only.
A program may use at most 128 MiB of HBM per device.

```python
import math
import jax
import jax.numpy as jnp
from jax import lax

D = 256
LAYERS = 4
SLOTS = 16
COLORS = 3
CELLS = 4
RAYS = 2048
SAMPLES = 64
N_CELL = 4


def touch_ends(result, rng, least, top_value):
    dims = result.shape
    index_at = [jax.random.randint(jax.random.fold_in(rng, axis), (), 0, dims[axis]) for axis in range(len(dims))]
    result = result.at[tuple(index_at)].set(least)
    longest = dims.index(max(dims))
    index_at[longest] = (index_at[longest] + 1) % dims[longest]
    return result.at[tuple(index_at)].set(top_value)


def levels(rng, extent, pieces, smallest, largest):
    def one(position, shards_of):
        heights = jax.random.uniform(jax.random.fold_in(jax.random.fold_in(rng, 6), position), (shards_of,), jnp.float32, smallest / len(pieces), largest / len(pieces))
        return jnp.repeat(jnp.exp(heights), extent[position] // shards_of).reshape((-1,) + (1,) * (len(extent) - position - 1))

    factor_of = one(*pieces[0])
    for cut in pieces[1:]:
        factor_of = factor_of * one(*cut)
    return factor_of


def centred(key, shape, deviation, most, shards=(), kind=jnp.bfloat16):
    drawn = jax.random.normal(key, shape, jnp.float32) * deviation
    if len(shards) > 0:
        drawn = levels(key, shape, shards, -0.22, 0.18) * drawn
    return jnp.clip(drawn, min=-most, max=most).astype(kind)


def setup_inputs(seed: int = 0) -> dict:
    streams_of = jax.random.split(jax.random.key(seed), 9)
    return {
        "encodings": centred(streams_of[0], (RAYS, SAMPLES, D), 1.0, 6.0, ((0, 8), (1, 4)), jnp.float32),
        "spacing": jnp.clip(jnp.exp(math.log(0.06) - 1.7917595 * jax.random.uniform(streams_of[1], (RAYS, SAMPLES), jnp.float32) ** levels(streams_of[1], (RAYS, SAMPLES), ((0, 8), (1, 4)), -0.2, 0.2)), 0.01, 0.06),
        "counts": touch_ends(jax.random.randint(streams_of[2], (RAYS, CELLS), 1, SLOTS + 1), jax.random.fold_in(streams_of[2], 1), 1, SLOTS).astype(jnp.int32),
        "cell_weights": centred(streams_of[3], (CELLS, LAYERS, D, D), D ** -0.5, 0.375, ((0, 4),), jnp.float32),
        "density_head": centred(streams_of[4], (CELLS, D), (D // 4) ** -0.5, 0.75, ((0, 4),), jnp.float32),
        "decoder_in": centred(streams_of[5], (D, D), (D // 4) ** -0.5, 0.75, (), jnp.float32),
        "decoder_out": centred(streams_of[6], (D, COLORS), D ** -0.5, 0.375, (), jnp.float32),
        "color_grad": centred(streams_of[7], (RAYS, COLORS), 0.05, 0.75, ((0, 8),), jnp.float32),
    }


HIGH = lax.Precision.HIGHEST


def silu_slope(pre):
    sig = jax.nn.sigmoid(pre)
    return sig * (1.0 + pre * (1.0 - sig))


def network(rows, weights):
    pres = []
    hidden = rows
    for layer in range(LAYERS):
        pre = jnp.dot(hidden, weights[layer], precision=HIGH, preferred_element_type=jnp.float32)
        pres.append(pre)
        hidden = jax.nn.silu(pre)
    return hidden, pres


def cell_rows(encodings, index):
    block = encodings[:, index * SLOTS:(index + 1) * SLOTS, :]
    return block.reshape(RAYS * SLOTS, D)


def reference(encodings, spacing, counts, cell_weights, density_head, decoder_in, decoder_out, color_grad):
    slot_ids = jnp.arange(SLOTS, dtype=jnp.int32)
    live = (slot_ids[None, None, :] < counts[:, :, None]).astype(jnp.float32).reshape(RAYS, SAMPLES)
    offset = jnp.zeros((RAYS,), jnp.float32)
    pixel = jnp.zeros((RAYS, D), jnp.float32)
    z_parts, tau_parts, trans_parts, weight_parts = [], [], [], []
    for index in range(N_CELL):
        hidden, _ = network(cell_rows(encodings, index), cell_weights[index])
        z = jnp.dot(hidden, density_head[index], precision=HIGH).reshape(RAYS, SLOTS)
        sel = slice(index * SLOTS, (index + 1) * SLOTS)
        tau = live[:, sel] * jax.nn.softplus(z) * spacing[:, sel]
        depth = offset[:, None] + jnp.cumsum(tau, axis=1) - tau
        trans = jnp.exp(-depth)
        weight = trans * (-jnp.expm1(-tau))
        offset = offset + jnp.sum(tau, axis=1)
        pixel = pixel + jnp.einsum("rs,rsd->rd", weight, hidden.reshape(RAYS, SLOTS, D), precision=HIGH)
        z_parts.append(z)
        tau_parts.append(tau)
        trans_parts.append(trans)
        weight_parts.append(weight)
    pre_dec = jnp.dot(pixel, decoder_in, precision=HIGH)
    act_dec = jax.nn.silu(pre_dec)
    decoder_out_grad = jnp.dot(act_dec.T, color_grad, precision=HIGH)
    dpre = jnp.dot(color_grad, decoder_out.T, precision=HIGH) * silu_slope(pre_dec)
    decoder_in_grad = jnp.dot(pixel.T, dpre, precision=HIGH)
    pixel_grad = jnp.dot(dpre, decoder_in.T, precision=HIGH)
    c_parts = []
    for index in range(N_CELL):
        hidden, _ = network(cell_rows(encodings, index), cell_weights[index])
        c_parts.append(jnp.einsum("rsd,rd->rs", hidden.reshape(RAYS, SLOTS, D), pixel_grad, precision=HIGH))
    c_all = jnp.concatenate(c_parts, axis=1)
    weight_all = jnp.concatenate(weight_parts, axis=1)
    weighted = weight_all * c_all
    after = jnp.sum(weighted, axis=1, keepdims=True) - jnp.cumsum(weighted, axis=1)
    layer_list, head_list, sample_list = [], [], []
    for index in range(N_CELL):
        sel = slice(index * SLOTS, (index + 1) * SLOTS)
        rows = cell_rows(encodings, index)
        hidden, pres = network(rows, cell_weights[index])
        dtau = trans_parts[index] * jnp.exp(-tau_parts[index]) * c_all[:, sel] - after[:, sel]
        dz = live[:, sel] * spacing[:, sel] * jax.nn.sigmoid(z_parts[index]) * dtau
        dz_rows = dz.reshape(RAYS * SLOTS)
        head_list.append(jnp.dot(dz_rows, hidden, precision=HIGH))
        back = (weight_parts[index][:, :, None] * pixel_grad[:, None, :]).reshape(RAYS * SLOTS, D)
        back = back + dz_rows[:, None] * density_head[index][None, :]
        grads = [None] * LAYERS
        for layer in reversed(range(LAYERS)):
            dp = back * silu_slope(pres[layer])
            source = rows if layer == 0 else jax.nn.silu(pres[layer - 1])
            grads[layer] = jnp.dot(source.T, dp, precision=HIGH)
            back = jnp.dot(dp, cell_weights[index, layer].T, precision=HIGH)
        layer_list.append(jnp.stack(grads))
        sample_list.append(back.reshape(RAYS, SLOTS, D))
    return (jnp.stack(layer_list), jnp.stack(head_list), decoder_in_grad, decoder_out_grad,
            jnp.concatenate(sample_list, axis=1))
```

```python
import jax
import jax.numpy as jnp
from jax import lax
from jax.experimental import pallas as pl
from jax.experimental.pallas import tpu as pltpu
from jax.sharding import PartitionSpec as P

HIGH = lax.Precision.HIGHEST
F32 = jnp.float32
BF16 = jnp.bfloat16
NN = ((1,), (0,))
NT = ((1,), (1,))
TN = ((0,), (0,))
SUB = 512
STEP = 2
PIECES = 2
VMEM = 58 << 20


def split(x):
    hi = x.astype(BF16)
    return hi, (x - hi.astype(F32)).astype(BF16)


def dot1(a, b, dims):
    return lax.dot_general(a, b, (dims, ((), ())), preferred_element_type=F32)


def dot3(a, b, dims):
    return dot1(a[0], b[0], dims) + dot1(a[0], b[1], dims) + dot1(a[1], b[0], dims)


def stacked(a, b, dims):
    n = a[0].shape[0]
    both = dot1(jnp.concatenate(a, axis=0), b[0], dims)
    return both[:n] + both[n:] + dot1(a[0], b[1], dims)


def sigmoid(x):
    return 0.5 * jnp.tanh(0.5 * x) + 0.5


def softplus(z):
    return jnp.maximum(z, 0.0) + jnp.log1p(jnp.exp(-jnp.abs(z)))


def one_minus_exp(tau):
    t = jnp.minimum(tau, 0.25)
    small = t * (1.0 - t / 2 * (1.0 - t / 3 * (1.0 - t / 4 * (1.0 - t / 5 * (1.0 - t / 6 * (1.0 - t / 7))))))
    return jnp.where(tau < 0.25, small, 1.0 - jnp.exp(-tau))


def ray_mask(rays, lanes, slots):
    r = lax.broadcasted_iota(jnp.int32, (rays, lanes), 0)
    c = lax.broadcasted_iota(jnp.int32, (rays, lanes), 1)
    return (c >= r * slots) & (c < r * slots + slots)


def slot_of(shape, slots):
    return lax.broadcasted_iota(jnp.int32, shape, 1) % slots


def scan_slots(x, slots, reverse=False):
    lanes = x.shape[1]
    slot = slot_of(x.shape, slots)
    k = 1
    while k < slots:
        if reverse:
            x = x + jnp.where(slot + k < slots, pltpu.roll(x, lanes - k, 1), 0.0)
        else:
            x = x + jnp.where(slot >= k, pltpu.roll(x, k, 1), 0.0)
        k *= 2
    return x


def column(row, rays):
    r = lax.broadcasted_iota(jnp.int32, (rays, rays), 0)
    c = lax.broadcasted_iota(jnp.int32, (rays, rays), 1)
    return jnp.sum(jnp.where(r == c, jnp.broadcast_to(row, (rays, rays)), 0.0), axis=1, keepdims=True)


def rows8(row):
    return jnp.broadcast_to(row, (8, row.shape[1]))


def spread(x, tr, slots):
    lanes = tr * slots
    t1, t2 = split(x)
    t3 = (x - t1.astype(F32) - t2.astype(F32)).astype(BF16)
    onto = ray_mask(tr, lanes, slots).astype(F32).astype(BF16)
    y = dot1(jnp.concatenate([t1, t2, t3], axis=0), onto, NN)
    y = y[:slots] + y[slots:2 * slots] + y[2 * slots:]
    own = lax.broadcasted_iota(jnp.int32, (slots, lanes), 1) % slots == lax.broadcasted_iota(jnp.int32, (slots, lanes), 0)
    return jnp.sum(jnp.where(own, y, 0.0), axis=0, keepdims=True)


def forward(slots, layers, steps):
    def body(enc, w, head, sp, cnt, *refs):
        pres, pext, refs = refs[:layers], refs[layers:layers + PIECES], refs[layers + PIECES:]
        zout, lsout, whi, wlo, hhi, hlo, pbuf, sems = refs
        i = pl.program_id(0)
        nsub = steps * STEP
        per = nsub // PIECES
        tr = SUB // slots
        nrays = per * tr
        blk = STEP * SUB

        def copy_out(l, k):
            rows = pl.ds(k * blk, blk)
            return pltpu.make_async_copy(pbuf.at[l, rows], pres[l].at[rows], sems.at[l, k])

        @pl.when(i == 0)
        def _():
            for l in range(layers):
                hi, lo = split(w[0, l])
                whi[l] = hi
                wlo[l] = lo

        cut = [slice(s * SUB, (s + 1) * SUB) for s in range(STEP)]
        h = [split(enc[c]) for c in cut]
        for l in range(layers):
            for s in range(STEP):
                p = dot3(h[s], (whi[l], wlo[l]), NN)
                pbuf[l, pl.ds(i * blk + s * SUB, SUB), :] = p
                h[s] = split(p * sigmoid(p))
        for l in range(layers):
            copy_out(l, i).start()
        hd = tuple(jnp.broadcast_to(x.astype(F32), (8, x.shape[1])).astype(BF16) for x in split(head[...]))
        for s in range(STEP):
            sub = i * STEP + s
            hhi[sub] = h[s][0]
            hlo[sub] = h[s][1]
            zout[pl.ds(sub, 1), :] = stacked(hd, h[s], NT)[:1]

        @pl.when(i == steps - 1)
        def _():
            live = lax.broadcasted_iota(jnp.int32, sp.shape, 0) < cnt[...]
            lst = jnp.where(live, sp[...], 0.0)
            for s in range(nsub):
                lsout[s:s + 1, :] = spread(lst[:, s * tr:(s + 1) * tr], tr, slots)
            mask = ray_mask(tr, SUB, slots)
            r = lax.broadcasted_iota(jnp.int32, (SUB, 128), 0)
            c = lax.broadcasted_iota(jnp.int32, (SUB, 128), 1)
            sums = jnp.where((r >= c * slots) & (r < c * slots + slots), 1.0, 0.0).astype(BF16)
            tau = lsout[...] * softplus(zout[...])
            incl = scan_slots(tau, slots)
            weight = jnp.exp(-(incl - tau)) * one_minus_exp(tau)
            for s in range(nsub):
                wm = jnp.where(mask, jnp.broadcast_to(weight[s:s + 1], (tr, SUB)), 0.0)
                r = (s % per) * tr
                pext[s // per][r:r + tr, :] = stacked(split(wm), (hhi[s], hlo[s]), NN)
            t1, t2 = split(tau)
            t3 = (tau - t1.astype(F32) - t2.astype(F32)).astype(BF16)
            total = dot1(jnp.concatenate([t1, t2, t3], axis=0), sums, NN)
            total = total[:nsub] + total[nsub:2 * nsub] + total[2 * nsub:]
            total = jnp.concatenate([total, jnp.zeros((nsub, pext[0].shape[1] - 128), F32)], axis=1)
            for q in range(PIECES):
                pext[q][nrays:, :] = jnp.zeros((8, total.shape[1]), F32)
                pext[q][nrays:nrays + per, :] = total[q * per:(q + 1) * per]
            for l in range(layers):
                for k in range(steps):
                    copy_out(l, k).wait()
    return body


def combine(tr):
    def body(flag, mine, other, total, suffix, off):
        n = mine.shape[0] - 8
        late = flag[0] == 1
        tm, to = mine[n:, :], other[n:, :]
        total[n:, :] = tm + to
        off[...] = jnp.where(late, to, 0.0)
        for s in range(n // tr):
            cut = slice(s * tr, (s + 1) * tr)
            a, b = mine[cut, :], other[cut, :]
            first = jnp.where(late, to[s:s + 1, :tr], tm[s:s + 1, :tr])
            e = jnp.exp(-column(first, tr))
            behind = jnp.where(late, a, b) * e
            total[cut, :] = jnp.where(late, b, a) + behind
            suffix[cut, :] = jnp.where(late, 0.0, behind)
    return body


def combine_more(tr):
    def body(flag, mine, other, suffix0, off0, total, suffix, off):
        n = mine.shape[0] - 8
        late = flag[0] == 1
        tm, to = mine[n:, :], other[n:, :]
        total[n:, :] = tm + to
        off[...] = jnp.where(late, to, 0.0) + off0[...]
        for s in range(n // tr):
            cut = slice(s * tr, (s + 1) * tr)
            a, b, sf = mine[cut, :], other[cut, :], suffix0[cut, :]
            first = jnp.where(late, to[s:s + 1, :tr], tm[s:s + 1, :tr])
            e = jnp.exp(-column(first, tr))
            total[cut, :] = jnp.where(late, b, a) + jnp.where(late, a, b) * e
            suffix[cut, :] = jnp.where(late, sf * e, sf + b * e)
    return body


def silu_parts(p):
    sig = sigmoid(p)
    h = p * sig
    return h, sig + h * (1.0 - sig)


def backward(slots, layers, steps):
    def body(flag, *refs):
        mines, others, suffixes, offs = (refs[k * PIECES:(k + 1) * PIECES] for k in range(4))
        din, dout, cg, w, head, ls, z, *refs = refs[4 * PIECES:]
        pres, enc, (sample, grads, gin, gsmall), refs = (
            refs[:layers], refs[layers], refs[layers + 1:layers + 5], refs[layers + 5:])
        wthi, wtlo, hhi, hlo, pg, cbuf, wbuf, dzbuf, small, later, ibuf, obuf, isems, osems = refs
        phase, i = pl.program_id(0), pl.program_id(1)
        tr = SUB // slots
        nsub = steps * STEP
        per = nsub // PIECES
        n = nsub * tr
        blk = STEP * SUB
        mask = ray_mask(tr, SUB, slots)
        sources = list(pres) + [enc]

        def copy_in(l, k):
            rows = pl.ds(k * blk, blk)
            return pltpu.make_async_copy(sources[l].at[rows], ibuf.at[l, rows], isems.at[l, k])

        def copy_out(k):
            rows = pl.ds(k * blk, blk)
            return pltpu.make_async_copy(obuf.at[rows], sample.at[rows], osems.at[k])

        def rows_of(s):
            return pl.ds(i * blk + s * SUB, SUB)

        @pl.when((phase == 0) & (i == 0))
        def _():
            for k in range(steps):
                copy_in(layers - 1, k).start()
            for k in range(steps):
                for l in list(reversed(range(layers - 1))) + [layers]:
                    copy_in(l, k).start()
            late = flag[0] == 1
            px, sx = [], []
            for s in range(nsub):
                q, t = s // per, s % per
                mine, other, suffix0, off0 = mines[q], others[q], suffixes[q], offs[q]
                at = slice(per * tr + t, per * tr + t + 1)
                to = other[at, :]
                first = jnp.where(late, to, mine[at, :])
                off = jnp.where(late, to, 0.0) + off0[t:t + 1, :]
                rc = slice(t * tr, (t + 1) * tr)
                a, b, sf = mine[rc, :], other[rc, :], suffix0[rc, :]
                e = jnp.exp(-column(first[:, :tr], tr))
                px.append(jnp.where(late, b, a) + jnp.where(late, a, b) * e)
                sx.append(jnp.where(late, sf * e, sf + b * e))
                offc = column(off[:, :tr], tr)
                later[s:s + 1, :] = jnp.sum(jnp.where(mask, offc, 0.0), axis=0, keepdims=True)
            px = split(jnp.concatenate(px, axis=0))
            small[...] = jnp.zeros(small.shape, F32)
            nc = cg.shape[0]
            small[:nc, :n] = cg[...]
            small[8:8 + nc, :dout.shape[1]] = dout[...]
            cg_t, dout_t = small[:8, :n], small[8:16, :dout.shape[1]]
            di = split(din[...])
            act, slope = silu_parts(dot3(px, di, NN))
            gsmall[...] = jnp.zeros(gsmall.shape, F32)
            gsmall[8:, :] = stacked(split(cg_t), split(act), NN)
            up = lax.dot_general(cg_t, dout_t, (TN, ((), ())), precision=HIGH, preferred_element_type=F32)
            dpre = split(up * slope)
            gin[...] = dot3(px, dpre, TN)
            g = dot3(dpre, di, NT)
            pg[...] = g
            for s in range(nsub):
                rc = slice(s * tr, (s + 1) * tr)
                lc = jnp.sum(sx[s] * g[rc, :], axis=1, keepdims=True)
                later[8 + s:9 + s, :] = jnp.sum(jnp.where(mask, lc, 0.0), axis=0, keepdims=True)
            for l in range(layers):
                hi, lo = split(w[0, l].T)
                wthi[l] = hi
                wtlo[l] = lo
            grads[...] = jnp.zeros(grads.shape, F32)

        @pl.when(phase == 0)
        def _():
            copy_in(layers - 1, i).wait()
            for s in range(STEP):
                sub = i * STEP + s
                p = ibuf[layers - 1, rows_of(s), :]
                h4 = split(p * sigmoid(p))
                hhi[sub] = h4[0]
                hlo[sub] = h4[1]
                g = pg[pl.ds(sub * tr, tr), :]
                c = stacked(split(g), h4, NT)
                cbuf[pl.ds(sub, 1), :] = jnp.sum(jnp.where(mask, c, 0.0), axis=0, keepdims=True)

        @pl.when((phase == 0) & (i == steps - 1))
        def _():
            slot = slot_of(z.shape, slots)
            zz, sp, c = z[...], ls[...], cbuf[...]
            tau = sp * softplus(zz)
            incl = scan_slots(tau, slots)
            trans = jnp.exp(-(later[:nsub, :] + (incl - tau)))
            weight = trans * one_minus_exp(tau)
            rest = scan_slots(weight * c, slots, reverse=True)
            after = later[8:8 + nsub, :] + jnp.where(slot + 1 < slots, pltpu.roll(rest, SUB - 1, 1), 0.0)
            dz = sp * jax.nn.sigmoid(zz) * (trans * jnp.exp(-tau) * c - after)
            wbuf[...] = weight
            dzbuf[...] = dz
            dh, dl = split(dz)
            acc = jnp.zeros((nsub, gsmall.shape[1]), F32)
            row = lax.broadcasted_iota(jnp.int32, dz.shape, 0)
            for s in range(nsub):
                d = tuple(jnp.where(row == s, x.astype(F32), 0.0).astype(BF16) for x in (dh, dl))
                acc = acc + stacked(d, (hhi[s], hlo[s]), NN)
            gsmall[:1, :] = jnp.sum(acc, axis=0, keepdims=True)

        @pl.when(phase == 1)
        def _():
            for l in list(range(layers - 1)) + [layers]:
                copy_in(l, i).wait()
            first = lax.broadcasted_iota(jnp.int32, (16, SUB), 0) == 0
            backs, slopes = [], []
            for s in range(STEP):
                sub = i * STEP + s
                g = pg[pl.ds(sub * tr, tr), :]
                a = jnp.concatenate([
                    jnp.where(mask, jnp.broadcast_to(wbuf[pl.ds(sub, 1), :], (tr, SUB)), 0.0),
                    jnp.where(first, jnp.broadcast_to(dzbuf[pl.ds(sub, 1), :], (16, SUB)), 0.0)], axis=0)
                b = jnp.concatenate([g, jnp.broadcast_to(head[...], (16, g.shape[1]))], axis=0)
                ah, al = split(a)
                bh, bl = split(b)
                backs.append(dot1(jnp.concatenate([ah, al, ah], axis=0), jnp.concatenate([bh, bh, bl], axis=0), TN))
                slopes.append(silu_parts(ibuf[layers - 1, rows_of(s), :])[1])
            for l in reversed(range(layers)):
                for s in range(STEP):
                    dp = split(backs[s] * slopes[s])
                    if l:
                        h, slopes[s] = silu_parts(ibuf[l - 1, rows_of(s), :])
                    else:
                        h = ibuf[layers, rows_of(s), :]
                    backs[s] = dot3(dp, (wthi[l], wtlo[l]), NN)
                    grads[l] += dot3(split(h), dp, TN)
            for s in range(STEP):
                obuf[rows_of(s), :] = backs[s]
            copy_out(i).start()

        @pl.when((phase == 1) & (i == steps - 1))
        def _():
            for k in range(steps):
                copy_out(k).wait()
    return body


def full(shape):
    return pl.BlockSpec(shape, lambda *_: (0,) * len(shape))


def call(body, grid, ins, outs, scratch=(), vmem=8 << 20):
    return pl.pallas_call(
        body,
        grid=grid,
        in_specs=list(ins),
        out_specs=[s for s, _ in outs],
        out_shape=[sh for _, sh in outs],
        scratch_shapes=list(scratch),
        compiler_params=pltpu.CompilerParams(vmem_limit_bytes=vmem),
    )


def arr(*shape):
    return jax.ShapeDtypeStruct(shape, F32)


def swap(x, axis, bit):
    return lax.ppermute(x, axis, [(i, i ^ bit) for i in range(lax.axis_size(axis))])


def bits_of(axis):
    n = lax.axis_size(axis)
    return [1 << k for k in range(n.bit_length() - 1)]


def all_reduce(pieces, axis):
    me = lax.axis_index(axis)
    bits = bits_of(axis)
    stages = [(b, True) for b in bits] + [(b, False) for b in reversed(bits)]
    pieces = list(pieces)
    for turn in range(len(stages) + len(pieces) - 1):
        for p in reversed(range(len(pieces))):
            if not 0 <= turn - p < len(stages):
                continue
            bit, halving = stages[turn - p]
            upper = (me // bit) % 2
            x = pieces[p]
            if halving:
                half = x.shape[0] // 2
                keep = lax.dynamic_slice_in_dim(x, upper * half, half)
                send = lax.dynamic_slice_in_dim(x, (1 - upper) * half, half)
                pieces[p] = keep + swap(send, axis, bit)
            else:
                got = swap(x, axis, bit)
                pieces[p] = jnp.where(upper == 1, jnp.concatenate([got, x]), jnp.concatenate([x, got]))
    return pieces


def local(encodings, spacing, counts, cell_weights, density_head, decoder_in, decoder_out, color_grad):
    rays, slots, width = encodings.shape
    layers = cell_weights.shape[1]
    total_rows = rays * slots
    tr = SUB // slots
    nsub = total_rows // SUB
    blk = STEP * SUB
    steps = total_rows // blk
    rows = encodings.reshape(total_rows, width)
    tile = pl.BlockSpec((blk, width), lambda i: (i, 0))
    wspec = full(cell_weights.shape)
    hspec = full((1, width))
    lane = full((nsub, SUB))
    prays = rays // PIECES
    ext = (prays + 8, width)
    hbm = pl.BlockSpec(memory_space=pl.ANY)
    *pres, z, ls = call(
        forward(slots, layers, steps), (steps,),
        [tile, wspec, hspec, full((slots, rays)), full((1, rays))],
        [(hbm, pltpu.HBM((total_rows, width), F32))] * layers
        + [(full(ext), arr(*ext))] * PIECES + [(lane, arr(nsub, SUB)), (lane, arr(nsub, SUB))],
        [pltpu.VMEM((layers, width, width), BF16)] * 2 + [pltpu.VMEM((nsub, SUB, width), BF16)] * 2
        + [pltpu.VMEM((layers, total_rows, width), F32), pltpu.SemaphoreType.DMA((layers, steps))],
        vmem=VMEM,
    )(rows, cell_weights, density_head, spacing.T, counts.T)
    pres, totals = pres[:layers], pres[layers:]

    me = lax.axis_index("cell")
    flat = full((prays, width))
    smem = pl.BlockSpec(memory_space=pltpu.SMEM)
    bits = bits_of("cell")
    suffixes = [jnp.zeros((prays, width), F32)] * PIECES
    offs = [jnp.zeros((8, width), F32)] * PIECES
    for k, bit in enumerate(bits):
        others = [swap(t, "cell", bit) for t in totals]
        flag = ((me // bit) % 2).astype(jnp.int32).reshape(1)
        if bit == bits[-1]:
            break
        outs = [(full(ext), arr(*ext)), (flat, arr(prays, width)), (full((8, width)), arr(8, width))]
        for q in range(PIECES):
            if k == 0:
                totals[q], suffixes[q], offs[q] = call(
                    combine(tr), (1,), [smem, full(ext), full(ext)], outs)(flag, totals[q], others[q])
            else:
                totals[q], suffixes[q], offs[q] = call(
                    combine_more(tr), (1,), [smem, full(ext), full(ext), flat, full((8, width))], outs
                )(flag, totals[q], others[q], suffixes[q], offs[q])

    colors = color_grad.shape[1]
    sq = (width, width)

    def once(shape):
        return pl.BlockSpec(shape, lambda p, i: (0,) * len(shape))

    gshape = (layers, width, width)
    sample, grads, gin, gsmall = call(
        backward(slots, layers, steps), (2, steps),
        [smem] + [once(ext)] * (2 * PIECES) + [once((prays, width))] * PIECES + [once((8, width))] * PIECES
        + [once(sq), once((colors, width)), once((colors, rays)), once(cell_weights.shape), once((1, width)),
           once((nsub, SUB)), once((nsub, SUB))] + [hbm] * (layers + 1),
        [(hbm, pltpu.HBM((total_rows, width), F32)), (once(gshape), arr(*gshape)), (once(sq), arr(*sq)),
         (once((16, width)), arr(16, width))],
        [pltpu.VMEM(gshape, BF16)] * 2 + [pltpu.VMEM((nsub, SUB, width), BF16)] * 2
        + [pltpu.VMEM((rays, width), F32)] + [pltpu.VMEM((nsub, SUB), F32)] * 3
        + [pltpu.VMEM((16, max(rays, width)), F32), pltpu.VMEM((16, SUB), F32)]
        + [pltpu.VMEM((layers + 1, total_rows, width), F32), pltpu.VMEM((total_rows, width), F32)]
        + [pltpu.SemaphoreType.DMA((layers + 1, steps)), pltpu.SemaphoreType.DMA((steps,))],
        vmem=VMEM,
    )(flag, *totals, *others, *suffixes, *offs, decoder_in, decoder_out.T, color_grad.T, cell_weights, density_head,
      ls, z, *pres, rows)

    flatg = grads.reshape(layers * width, width)
    n = layers * width // 2
    first, second = all_reduce([
        jnp.concatenate([flatg[n:], gin[:width // 2], gsmall, jnp.zeros((48, width), F32)]),
        jnp.concatenate([flatg[:n], gin[width // 2:]]),
    ], "rays")
    m = n + width // 2
    return (
        jnp.concatenate([second[:n], first[:n]]).reshape(1, layers, width, width),
        first[m:m + 1],
        jnp.concatenate([first[n:m], second[n:m]]),
        first[m + 8:m + 8 + colors].T,
        sample.reshape(rays, slots, width),
    )


def solution(mesh):
    in_specs = (
        P("rays", "cell", None),
        P("rays", "cell"),
        P("rays", "cell"),
        P("cell", None, None, None),
        P("cell", None),
        P(),
        P(),
        P("rays", None),
    )
    out_specs = (P("cell", None, None, None), P("cell", None), P(), P(), P("rays", "cell", None))
    return jax.shard_map(local, mesh=mesh, in_specs=in_specs, out_specs=out_specs, check_vma=False)
```

```python
import jax
import jax.numpy as jnp
from jax import lax
from jax.experimental import pallas as pl
from jax.experimental.pallas import tpu as pltpu
from jax.sharding import PartitionSpec as P

HIGH = lax.Precision.HIGHEST
F32 = jnp.float32
BF16 = jnp.bfloat16
NN = ((1,), (0,))
NT = ((1,), (1,))
TN = ((0,), (0,))
SUB = 512
STEP = 4
PIECES = 2
SKEW = 0
VMEM_F = 42 << 20
VMEM_B = 48 << 20


def split(x):
    hi = x.astype(BF16)
    return hi, (x - hi.astype(F32)).astype(BF16)


def dot1(a, b, dims):
    return lax.dot_general(a, b, (dims, ((), ())), preferred_element_type=F32)


def dot3(a, b, dims):
    return dot1(a[0], b[0], dims) + dot1(a[0], b[1], dims) + dot1(a[1], b[0], dims)


def stacked(a, b, dims):
    n = a[0].shape[0]
    both = dot1(jnp.concatenate(a, axis=0), b[0], dims)
    return both[:n] + both[n:] + dot1(a[0], b[1], dims)


def sigmoid(x):
    return 0.5 * jnp.tanh(0.5 * x) + 0.5


def softplus(z):
    return jnp.maximum(z, 0.0) + jnp.log1p(jnp.exp(-jnp.abs(z)))


def one_minus_exp(tau):
    t = jnp.minimum(tau, 0.25)
    small = t * (1.0 - t / 2 * (1.0 - t / 3 * (1.0 - t / 4 * (1.0 - t / 5 * (1.0 - t / 6 * (1.0 - t / 7))))))
    return jnp.where(tau < 0.25, small, 1.0 - jnp.exp(-tau))


def ray_mask(rays, lanes, slots):
    r = lax.broadcasted_iota(jnp.int32, (rays, lanes), 0)
    c = lax.broadcasted_iota(jnp.int32, (rays, lanes), 1)
    return (c >= r * slots) & (c < r * slots + slots)


def slot_of(shape, slots):
    return lax.broadcasted_iota(jnp.int32, shape, 1) % slots


def scan_slots(x, slots, reverse=False):
    lanes = x.shape[1]
    slot = slot_of(x.shape, slots)
    k = 1
    while k < slots:
        if reverse:
            x = x + jnp.where(slot + k < slots, pltpu.roll(x, lanes - k, 1), 0.0)
        else:
            x = x + jnp.where(slot >= k, pltpu.roll(x, k, 1), 0.0)
        k *= 2
    return x


def column(row, rays):
    r = lax.broadcasted_iota(jnp.int32, (rays, rays), 0)
    c = lax.broadcasted_iota(jnp.int32, (rays, rays), 1)
    return jnp.sum(jnp.where(r == c, jnp.broadcast_to(row, (rays, rays)), 0.0), axis=1, keepdims=True)


def rows8(row):
    return jnp.broadcast_to(row, (8, row.shape[1]))


def spread(x, tr, slots):
    lanes = tr * slots
    t1, t2 = split(x)
    t3 = (x - t1.astype(F32) - t2.astype(F32)).astype(BF16)
    onto = ray_mask(tr, lanes, slots).astype(F32).astype(BF16)
    y = dot1(jnp.concatenate([t1, t2, t3], axis=0), onto, NN)
    y = y[:slots] + y[slots:2 * slots] + y[2 * slots:]
    own = lax.broadcasted_iota(jnp.int32, (slots, lanes), 1) % slots == lax.broadcasted_iota(jnp.int32, (slots, lanes), 0)
    return jnp.sum(jnp.where(own, y, 0.0), axis=0, keepdims=True)


def forward(slots, layers, steps):
    def body(enc, w, head, sp, cnt, *refs):
        pres, pext, refs = refs[:layers], refs[layers:layers + PIECES], refs[layers + PIECES:]
        zout, lsout, whi, wlo, hhi, hlo, pbuf, sems = refs
        i = pl.program_id(0)
        nsub = steps * STEP
        per = nsub // PIECES
        tr = SUB // slots
        nrays = per * tr
        blk = STEP * SUB

        def copy_out(l, k):
            rows = pl.ds(k * blk, blk)
            return pltpu.make_async_copy(pbuf.at[l, rows], pres[l].at[rows], sems.at[l, k])

        @pl.when(i == 0)
        def _():
            for l in range(layers):
                hi, lo = split(w[0, l])
                whi[l] = hi
                wlo[l] = lo

        cut = [slice(s * SUB, (s + 1) * SUB) for s in range(STEP)]
        h = [split(enc[c]) for c in cut]
        for l in range(layers):
            for s in range(STEP):
                p = dot3(h[s], (whi[l], wlo[l]), NN)
                pbuf[l, pl.ds(i * blk + s * SUB, SUB), :] = p
                h[s] = split(p * sigmoid(p))
            copy_out(l, i).start()
        hd = tuple(jnp.broadcast_to(x.astype(F32), (8, x.shape[1])).astype(BF16) for x in split(head[...]))
        for s in range(STEP):
            sub = i * STEP + s
            hhi[sub] = h[s][0]
            hlo[sub] = h[s][1]
            zout[pl.ds(sub, 1), :] = stacked(hd, h[s], NT)[:1]

        @pl.when(i == steps - 1)
        def _():
            live = lax.broadcasted_iota(jnp.int32, sp.shape, 0) < cnt[...]
            lst = jnp.where(live, sp[...], 0.0)
            for s in range(nsub):
                lsout[s:s + 1, :] = spread(lst[:, s * tr:(s + 1) * tr], tr, slots)
            mask = ray_mask(tr, SUB, slots)
            r = lax.broadcasted_iota(jnp.int32, (SUB, 128), 0)
            c = lax.broadcasted_iota(jnp.int32, (SUB, 128), 1)
            sums = jnp.where((r >= c * slots) & (r < c * slots + slots), 1.0, 0.0).astype(BF16)
            tau = lsout[...] * softplus(zout[...])
            incl = scan_slots(tau, slots)
            weight = jnp.exp(-(incl - tau)) * one_minus_exp(tau)
            for s in range(nsub):
                wm = jnp.where(mask, jnp.broadcast_to(weight[s:s + 1], (tr, SUB)), 0.0)
                r = (s % per) * tr
                pext[s // per][r:r + tr, :] = stacked(split(wm), (hhi[s], hlo[s]), NN)
            t1, t2 = split(tau)
            t3 = (tau - t1.astype(F32) - t2.astype(F32)).astype(BF16)
            total = dot1(jnp.concatenate([t1, t2, t3], axis=0), sums, NN)
            total = total[:nsub] + total[nsub:2 * nsub] + total[2 * nsub:]
            total = jnp.concatenate([total, jnp.zeros((nsub, pext[0].shape[1] - 128), F32)], axis=1)
            for q in range(PIECES):
                pext[q][nrays:, :] = jnp.zeros((8, total.shape[1]), F32)
                pext[q][nrays:nrays + per, :] = total[q * per:(q + 1) * per]
            for l in range(layers):
                for k in range(steps):
                    copy_out(l, k).wait()
    return body


def combine(stage, tr):
    def body(flags, mine, other, total):
        per = mine.shape[0] - 8
        late = flags[stage] == 1
        tm, to = mine[per:, :], other[per:, :]
        total[per:, :] = tm + to
        for s in range(per // tr):
            cut = slice(s * tr, (s + 1) * tr)
            a, b = mine[cut, :], other[cut, :]
            first = jnp.where(late, to[s:s + 1, :tr], tm[s:s + 1, :tr])
            total[cut, :] = jnp.where(late, b, a) + jnp.where(late, a, b) * jnp.exp(-column(first, tr))
    return body


def silu_parts(p):
    sig = sigmoid(p)
    h = p * sig
    return h, sig + h * (1.0 - sig)


def backward(slots, layers, steps, stages):
    def body(flags, *refs):
        mines, refs = refs[:PIECES], refs[PIECES:]
        others, refs = [refs[k * PIECES:(k + 1) * PIECES] for k in range(stages)], refs[stages * PIECES:]
        din, dout, cg, w, head, ls, z, *refs = refs
        pres, enc, (sample, g1, g2), refs = refs[:layers], refs[layers], refs[layers + 1:layers + 4], refs[layers + 4:]
        wthi, wtlo, hhi, hlo, pg, cbuf, wbuf, dzbuf, small, later, ibuf, obuf, isems, osems = refs
        width = pg.shape[1]
        top = (layers // 2) * width
        tail = top + width // 2
        per_rays = mines[0].shape[0] - 8

        def add_grad(l, g):
            ref = g1 if l >= layers // 2 else g2
            rows = slice((l % (layers // 2)) * width, (l % (layers // 2) + 1) * width)
            ref[rows, :] += g

        phase, i = pl.program_id(0), pl.program_id(1)
        tr = SUB // slots
        nsub = steps * STEP
        per = nsub // PIECES
        n = nsub * tr
        blk = STEP * SUB
        mask = ray_mask(tr, SUB, slots)
        sources = list(pres) + [enc]

        def copy_in(l, k):
            rows = pl.ds(k * blk, blk)
            return pltpu.make_async_copy(sources[l].at[rows], ibuf.at[l, rows], isems.at[l, k])

        def copy_out(k):
            rows = pl.ds(k * blk, blk)
            return pltpu.make_async_copy(obuf.at[rows], sample.at[rows], osems.at[k])

        def rows_of(s):
            return pl.ds(i * blk + s * SUB, SUB)

        @pl.when((phase == 0) & (i == 0))
        def _():
            for k in range(steps):
                copy_in(layers - 1, k).start()
            for k in range(steps):
                for l in list(reversed(range(layers - 1))) + [layers]:
                    copy_in(l, k).start()
            px, sx = [], []
            for s in range(nsub):
                q, t = s // per, s % per
                at = slice(per_rays + t, per_rays + t + 1)
                rc = slice(t * tr, (t + 1) * tr)
                a, mt = mines[q][rc, :], mines[q][at, :]
                sf, off = jnp.zeros(a.shape, F32), jnp.zeros(mt.shape, F32)
                for k in range(stages):
                    late = flags[k] == 1
                    b, to = others[k][q][rc, :], others[k][q][at, :]
                    e = jnp.exp(-column(jnp.where(late, to, mt)[:, :tr], tr))
                    sf = jnp.where(late, sf * e, sf + b * e)
                    off = off + jnp.where(late, to, 0.0)
                    a, mt = jnp.where(late, b, a) + jnp.where(late, a, b) * e, mt + to
                px.append(a)
                sx.append(sf)
                offc = column(off[:, :tr], tr)
                later[s:s + 1, :] = jnp.sum(jnp.where(mask, offc, 0.0), axis=0, keepdims=True)
            px = split(jnp.concatenate(px, axis=0))
            small[...] = jnp.zeros(small.shape, F32)
            nc = cg.shape[0]
            small[:nc, :n] = cg[...]
            small[8:8 + nc, :dout.shape[1]] = dout[...]
            cg_t, dout_t = small[:8, :n], small[8:16, :dout.shape[1]]
            di = split(din[...])
            act, slope = silu_parts(dot3(px, di, NN))
            g1[...] = jnp.zeros(g1.shape, F32)
            g2[...] = jnp.zeros(g2.shape, F32)
            g1[tail + 8:tail + 16, :] = stacked(split(cg_t), split(act), NN)
            up = lax.dot_general(cg_t, dout_t, (TN, ((), ())), precision=HIGH, preferred_element_type=F32)
            dpre = split(up * slope)
            gin = dot3(px, dpre, TN)
            g1[top:tail, :] = gin[:width // 2]
            g2[top:tail, :] = gin[width // 2:]
            g = dot3(dpre, di, NT)
            pg[...] = g
            for s in range(nsub):
                rc = slice(s * tr, (s + 1) * tr)
                lc = jnp.sum(sx[s] * g[rc, :], axis=1, keepdims=True)
                later[8 + s:9 + s, :] = jnp.sum(jnp.where(mask, lc, 0.0), axis=0, keepdims=True)
            for l in range(layers):
                hi, lo = split(w[0, l].T)
                wthi[l] = hi
                wtlo[l] = lo

        @pl.when(phase == 0)
        def _():
            copy_in(layers - 1, i).wait()
            for s in range(STEP):
                sub = i * STEP + s
                p = ibuf[layers - 1, rows_of(s), :]
                h4 = split(p * sigmoid(p))
                hhi[sub] = h4[0]
                hlo[sub] = h4[1]
                g = pg[pl.ds(sub * tr, tr), :]
                c = stacked(split(g), h4, NT)
                cbuf[pl.ds(sub, 1), :] = jnp.sum(jnp.where(mask, c, 0.0), axis=0, keepdims=True)

        @pl.when((phase == 0) & (i == steps - 1))
        def _():
            slot = slot_of(z.shape, slots)
            zz, sp, c = z[...], ls[...], cbuf[...]
            tau = sp * softplus(zz)
            incl = scan_slots(tau, slots)
            trans = jnp.exp(-(later[:nsub, :] + (incl - tau)))
            weight = trans * one_minus_exp(tau)
            rest = scan_slots(weight * c, slots, reverse=True)
            after = later[8:8 + nsub, :] + jnp.where(slot + 1 < slots, pltpu.roll(rest, SUB - 1, 1), 0.0)
            dz = sp * jax.nn.sigmoid(zz) * (trans * jnp.exp(-tau) * c - after)
            wbuf[...] = weight
            dzbuf[...] = dz
            dh, dl = split(dz)
            acc = jnp.zeros((nsub, width), F32)
            row = lax.broadcasted_iota(jnp.int32, dz.shape, 0)
            for s in range(nsub):
                d = tuple(jnp.where(row == s, x.astype(F32), 0.0).astype(BF16) for x in (dh, dl))
                acc = acc + stacked(d, (hhi[s], hlo[s]), NN)
            g1[tail:tail + 1, :] = jnp.sum(acc, axis=0, keepdims=True)

        @pl.when(phase == 1)
        def _():
            for l in list(range(layers - 1)) + [layers]:
                copy_in(l, i).wait()
            first = lax.broadcasted_iota(jnp.int32, (16, SUB), 0) == 0
            backs, slopes = [], []
            for s in range(STEP):
                sub = i * STEP + s
                g = pg[pl.ds(sub * tr, tr), :]
                a = jnp.concatenate([
                    jnp.where(mask, jnp.broadcast_to(wbuf[pl.ds(sub, 1), :], (tr, SUB)), 0.0),
                    jnp.where(first, jnp.broadcast_to(dzbuf[pl.ds(sub, 1), :], (16, SUB)), 0.0)], axis=0)
                b = jnp.concatenate([g, jnp.broadcast_to(head[...], (16, g.shape[1]))], axis=0)
                ah, al = split(a)
                bh, bl = split(b)
                backs.append(dot1(jnp.concatenate([ah, al, ah], axis=0), jnp.concatenate([bh, bh, bl], axis=0), TN))
                slopes.append(silu_parts(ibuf[layers - 1, rows_of(s), :])[1])
            for l in reversed(range(layers)):
                for s in range(STEP):
                    dp = split(backs[s] * slopes[s])
                    if l:
                        h, slopes[s] = silu_parts(ibuf[l - 1, rows_of(s), :])
                    else:
                        h = ibuf[layers, rows_of(s), :]
                    backs[s] = dot3(dp, (wthi[l], wtlo[l]), NN)
                    if l == 0:
                        obuf[rows_of(s), :] = backs[s]
                    if l == 0 and s == STEP - 1:
                        copy_out(i).start()
                    add_grad(l, dot3(split(h), dp, TN))

        @pl.when((phase == 1) & (i == steps - 1))
        def _():
            for k in range(steps):
                copy_out(k).wait()
    return body


def finish(layers, width, colors):
    def body(flag, x1, got1, x2, got2, lg, hg, gin, gout):
        upper = flag[0] == 1
        half = layers // 2
        top, tail = half * width, half * width + width // 2

        def rows(piece, a, b):
            x, got = piece
            m = x.shape[0]
            parts = []
            if a < m:
                cut = slice(a, min(b, m))
                parts.append(jnp.where(upper, got[cut, :], x[cut, :]))
            if b > m:
                cut = slice(max(a, m) - m, b - m)
                parts.append(jnp.where(upper, x[cut, :], got[cut, :]))
            return parts[0] if len(parts) == 1 else jnp.concatenate(parts, axis=0)

        for l in range(layers):
            piece = (x1, got1) if l >= half else (x2, got2)
            lg[0, l] = rows(piece, (l % half) * width, (l % half + 1) * width)
        gin[:width // 2, :] = rows((x1, got1), top, tail)
        gin[width // 2:, :] = rows((x2, got2), top, tail)
        end = rows((x1, got1), tail, tail + 16)
        hg[...] = end[:1]
        gout[...] = end[8:8 + colors]
    return body


def pinned(x):
    return pltpu.with_memory_space_constraint(x, pltpu.HBM)


def full(shape):
    return pl.BlockSpec(shape, lambda *_: (0,) * len(shape))


def call(body, grid, ins, outs, scratch=(), vmem=8 << 20):
    return pl.pallas_call(
        body,
        grid=grid,
        in_specs=list(ins),
        out_specs=[s for s, _ in outs],
        out_shape=[sh for _, sh in outs],
        scratch_shapes=list(scratch),
        compiler_params=pltpu.CompilerParams(vmem_limit_bytes=vmem),
    )


def arr(*shape):
    return jax.ShapeDtypeStruct(shape, F32)


def swap(x, axis, bit):
    return lax.ppermute(x, axis, [(i, i ^ bit) for i in range(lax.axis_size(axis))])


def bits_of(axis):
    n = lax.axis_size(axis)
    return [1 << k for k in range(n.bit_length() - 1)]


def all_reduce(pieces, axis):
    me = lax.axis_index(axis)
    bits = bits_of(axis)
    pieces = list(pieces)
    plans = []
    for p in range(len(pieces)):
        order = bits if p == 0 else bits[:1] + bits[:0:-1]
        plans.append([(b, True) for b in order] + [(b, False) for b in reversed(order)])
    for turn in range(len(plans[0]) + SKEW * (len(pieces) - 1)):
        for p in reversed(range(len(pieces))):
            stages = plans[p]
            if not 0 <= turn - SKEW * p < len(stages):
                continue
            bit, halving = stages[turn - SKEW * p]
            upper = (me // bit) % 2
            x = pieces[p]
            if halving:
                half = x.shape[0] // 2
                keep = lax.dynamic_slice_in_dim(x, upper * half, half)
                send = lax.dynamic_slice_in_dim(x, (1 - upper) * half, half)
                pieces[p] = keep + swap(send, axis, bit)
            else:
                got = swap(x, axis, bit)
                if turn - SKEW * p == len(stages) - 1:
                    pieces[p] = (x, got)
                    continue
                pieces[p] = jnp.where(upper == 1, jnp.concatenate([got, x]), jnp.concatenate([x, got]))
    return pieces


def local(encodings, spacing, counts, cell_weights, density_head, decoder_in, decoder_out, color_grad):
    rays, slots, width = encodings.shape
    layers = cell_weights.shape[1]
    total_rows = rays * slots
    tr = SUB // slots
    nsub = total_rows // SUB
    blk = STEP * SUB
    steps = total_rows // blk
    rows = pinned(encodings.reshape(total_rows, width))
    weights = pinned(cell_weights)
    tile = pl.BlockSpec((blk, width), lambda i: (i, 0))
    wspec = full(cell_weights.shape)
    hspec = full((1, width))
    lane = full((nsub, SUB))
    prays = rays // PIECES
    ext = (prays + 8, width)
    hbm = pl.BlockSpec(memory_space=pl.ANY)
    *pres, z, ls = call(
        forward(slots, layers, steps), (steps,),
        [tile, wspec, hspec, full((slots, rays)), full((1, rays))],
        [(hbm, pltpu.HBM((total_rows, width), F32))] * layers
        + [(full(ext), arr(*ext))] * PIECES + [(lane, arr(nsub, SUB)), (lane, arr(nsub, SUB))],
        [pltpu.VMEM((layers, width, width), BF16)] * 2 + [pltpu.VMEM((nsub, SUB, width), BF16)] * 2
        + [pltpu.VMEM((layers, total_rows, width), F32), pltpu.SemaphoreType.DMA((layers, steps))],
        vmem=VMEM_F,
    )(rows, weights, pinned(density_head), pinned(spacing.T), pinned(counts.T))
    pres, totals = pres[:layers], pres[layers:]

    me = lax.axis_index("cell")
    smem = pl.BlockSpec(memory_space=pltpu.SMEM)
    bits = bits_of("cell")
    flags = jnp.stack([(me // bit) % 2 for bit in bits]).astype(jnp.int32)
    mines, others = list(totals), []
    for k, bit in enumerate(bits):
        others.append([swap(t, "cell", bit) for t in totals])
        if bit != bits[-1]:
            totals = [
                call(combine(k, tr), (1,), [smem, full(ext), full(ext)], [(full(ext), arr(*ext))])(flags, t, o)[0]
                for t, o in zip(totals, others[-1])]

    colors = color_grad.shape[1]
    sq = (width, width)

    def once(shape):
        return pl.BlockSpec(shape, lambda p, i: (0,) * len(shape))

    gshape = (layers, width, width)
    top = (layers // 2) * width + width // 2
    shape1, shape2 = (top + 64, width), (top, width)
    sample, g1, g2 = call(
        backward(slots, layers, steps, len(bits)), (2, steps),
        [smem] + [once(ext)] * (PIECES * (1 + len(bits)))
        + [once(sq), once((colors, width)), once((colors, rays)), once(cell_weights.shape), once((1, width)),
           once((nsub, SUB)), once((nsub, SUB))] + [hbm] * (layers + 1),
        [(hbm, pltpu.HBM((total_rows, width), F32)), (once(shape1), arr(*shape1)), (once(shape2), arr(*shape2))],
        [pltpu.VMEM(gshape, BF16)] * 2 + [pltpu.VMEM((nsub, SUB, width), BF16)] * 2
        + [pltpu.VMEM((rays, width), F32)] + [pltpu.VMEM((nsub, SUB), F32)] * 3
        + [pltpu.VMEM((16, max(rays, width)), F32), pltpu.VMEM((16, SUB), F32)]
        + [pltpu.VMEM((layers + 1, total_rows, width), F32), pltpu.VMEM((total_rows, width), F32)]
        + [pltpu.SemaphoreType.DMA((layers + 1, steps)), pltpu.SemaphoreType.DMA((steps,))],
        vmem=VMEM_B,
    )(flags, *mines, *[o for group in others for o in group], decoder_in, decoder_out.T, color_grad.T, weights,
      density_head, ls, z, *pres, rows)

    pieces = all_reduce([g1, g2], "rays")
    flag = (lax.axis_index("rays") % 2).astype(jnp.int32).reshape(1)
    h1, h2 = (top + 64) // 2, top // 2
    layer_grads, head_grads, din_grad, dout_grad = call(
        finish(layers, width, colors), (1,),
        [smem, full((h1, width)), full((h1, width)), full((h2, width)), full((h2, width))],
        [(full(cell_weights.shape), arr(*cell_weights.shape)), (full((1, width)), arr(1, width)), (full(sq), arr(*sq)),
         (full((colors, width)), arr(colors, width))], vmem=16 << 20,
    )(flag, *pieces[0], *pieces[1])
    return layer_grads, head_grads, din_grad, dout_grad.T, sample.reshape(rays, slots, width)


def solution(mesh):
    in_specs = (
        P("rays", "cell", None),
        P("rays", "cell"),
        P("rays", "cell"),
        P("cell", None, None, None),
        P("cell", None),
        P(),
        P(),
        P("rays", None),
    )
    out_specs = (P("cell", None, None, None), P("cell", None), P(), P(), P("rays", "cell", None))
    return jax.shard_map(local, mesh=mesh, in_specs=in_specs, out_specs=out_specs, check_vma=False)
```

```python
import jax
import jax.numpy as jnp
from jax import lax
from jax.experimental import pallas as pl
from jax.experimental.pallas import tpu as pltpu
from jax.sharding import PartitionSpec as P

HIGH = lax.Precision.HIGHEST
F32 = jnp.float32
BF16 = jnp.bfloat16
NN = ((1,), (0,))
NT = ((1,), (1,))
TN = ((0,), (0,))
SUB = 512
STEP = 4
PIECES = 4
SKEW = 0
VMEM_F = 42 << 20
VMEM_B = 48 << 20


def split(x):
    hi = x.astype(BF16)
    return hi, (x - hi.astype(F32)).astype(BF16)


def dot1(a, b, dims):
    return lax.dot_general(a, b, (dims, ((), ())), preferred_element_type=F32)


def dot3(a, b, dims):
    return dot1(a[0], b[0], dims) + dot1(a[0], b[1], dims) + dot1(a[1], b[0], dims)


def stacked(a, b, dims):
    n = a[0].shape[0]
    both = dot1(jnp.concatenate(a, axis=0), b[0], dims)
    return both[:n] + both[n:] + dot1(a[0], b[1], dims)


def sigmoid(x):
    return 0.5 * jnp.tanh(0.5 * x) + 0.5


def softplus(z):
    return jnp.maximum(z, 0.0) + jnp.log1p(jnp.exp(-jnp.abs(z)))


def one_minus_exp(tau):
    t = jnp.minimum(tau, 0.25)
    small = t * (1.0 - t / 2 * (1.0 - t / 3 * (1.0 - t / 4 * (1.0 - t / 5 * (1.0 - t / 6 * (1.0 - t / 7))))))
    return jnp.where(tau < 0.25, small, 1.0 - jnp.exp(-tau))


def ray_mask(rays, lanes, slots):
    r = lax.broadcasted_iota(jnp.int32, (rays, lanes), 0)
    c = lax.broadcasted_iota(jnp.int32, (rays, lanes), 1)
    return (c >= r * slots) & (c < r * slots + slots)


def slot_of(shape, slots):
    return lax.broadcasted_iota(jnp.int32, shape, 1) % slots


def scan_slots(x, slots, reverse=False):
    lanes = x.shape[1]
    slot = slot_of(x.shape, slots)
    k = 1
    while k < slots:
        if reverse:
            x = x + jnp.where(slot + k < slots, pltpu.roll(x, lanes - k, 1), 0.0)
        else:
            x = x + jnp.where(slot >= k, pltpu.roll(x, k, 1), 0.0)
        k *= 2
    return x


def column(row, rays):
    r = lax.broadcasted_iota(jnp.int32, (rays, rays), 0)
    c = lax.broadcasted_iota(jnp.int32, (rays, rays), 1)
    return jnp.sum(jnp.where(r == c, jnp.broadcast_to(row, (rays, rays)), 0.0), axis=1, keepdims=True)


def rows8(row):
    return jnp.broadcast_to(row, (8, row.shape[1]))


def spread(x, tr, slots):
    lanes = tr * slots
    t1, t2 = split(x)
    t3 = (x - t1.astype(F32) - t2.astype(F32)).astype(BF16)
    onto = ray_mask(tr, lanes, slots).astype(F32).astype(BF16)
    y = dot1(jnp.concatenate([t1, t2, t3], axis=0), onto, NN)
    y = y[:slots] + y[slots:2 * slots] + y[2 * slots:]
    own = lax.broadcasted_iota(jnp.int32, (slots, lanes), 1) % slots == lax.broadcasted_iota(jnp.int32, (slots, lanes), 0)
    return jnp.sum(jnp.where(own, y, 0.0), axis=0, keepdims=True)


def forward(slots, layers, steps):
    def body(enc, w, head, sp, cnt, *refs):
        pres, pext, refs = refs[:layers], refs[layers:layers + PIECES], refs[layers + PIECES:]
        zout, lsout, whi, wlo, hhi, hlo, pbuf, sems = refs
        i = pl.program_id(0)
        nsub = steps * STEP
        per = nsub // PIECES
        tr = SUB // slots
        nrays = per * tr
        blk = STEP * SUB

        def copy_out(l, k):
            rows = pl.ds(k * blk, blk)
            return pltpu.make_async_copy(pbuf.at[l, rows], pres[l].at[rows], sems.at[l, k])

        @pl.when(i == 0)
        def _():
            for l in range(layers):
                hi, lo = split(w[0, l])
                whi[l] = hi
                wlo[l] = lo

        cut = [slice(s * SUB, (s + 1) * SUB) for s in range(STEP)]
        h = [split(enc[c]) for c in cut]
        for l in range(layers):
            for s in range(STEP):
                p = dot3(h[s], (whi[l], wlo[l]), NN)
                pbuf[l, pl.ds(i * blk + s * SUB, SUB), :] = p
                h[s] = split(p * sigmoid(p))
            copy_out(l, i).start()
        hd = tuple(jnp.broadcast_to(x.astype(F32), (8, x.shape[1])).astype(BF16) for x in split(head[...]))
        for s in range(STEP):
            sub = i * STEP + s
            hhi[sub] = h[s][0]
            hlo[sub] = h[s][1]
            zout[pl.ds(sub, 1), :] = stacked(hd, h[s], NT)[:1]

        @pl.when(i == steps - 1)
        def _():
            live = lax.broadcasted_iota(jnp.int32, sp.shape, 0) < cnt[...]
            lst = jnp.where(live, sp[...], 0.0)
            for s in range(nsub):
                lsout[s:s + 1, :] = spread(lst[:, s * tr:(s + 1) * tr], tr, slots)
            mask = ray_mask(tr, SUB, slots)
            r = lax.broadcasted_iota(jnp.int32, (SUB, 128), 0)
            c = lax.broadcasted_iota(jnp.int32, (SUB, 128), 1)
            sums = jnp.where((r >= c * slots) & (r < c * slots + slots), 1.0, 0.0).astype(BF16)
            tau = lsout[...] * softplus(zout[...])
            incl = scan_slots(tau, slots)
            weight = jnp.exp(-(incl - tau)) * one_minus_exp(tau)
            for s in range(nsub):
                wm = jnp.where(mask, jnp.broadcast_to(weight[s:s + 1], (tr, SUB)), 0.0)
                r = (s % per) * tr
                pext[s // per][r:r + tr, :] = stacked(split(wm), (hhi[s], hlo[s]), NN)
            t1, t2 = split(tau)
            t3 = (tau - t1.astype(F32) - t2.astype(F32)).astype(BF16)
            total = dot1(jnp.concatenate([t1, t2, t3], axis=0), sums, NN)
            total = total[:nsub] + total[nsub:2 * nsub] + total[2 * nsub:]
            total = jnp.concatenate([total, jnp.zeros((nsub, pext[0].shape[1] - 128), F32)], axis=1)
            for q in range(PIECES):
                pext[q][nrays:, :] = jnp.zeros((8, total.shape[1]), F32)
                pext[q][nrays:nrays + per, :] = total[q * per:(q + 1) * per]
            for l in range(layers):
                for k in range(steps):
                    copy_out(l, k).wait()
    return body


def combine(stage, tr):
    def body(flags, mine, other, total):
        per = mine.shape[0] - 8
        late = flags[stage] == 1
        tm, to = mine[per:, :], other[per:, :]
        total[per:, :] = tm + to
        for s in range(per // tr):
            cut = slice(s * tr, (s + 1) * tr)
            a, b = mine[cut, :], other[cut, :]
            first = jnp.where(late, to[s:s + 1, :tr], tm[s:s + 1, :tr])
            total[cut, :] = jnp.where(late, b, a) + jnp.where(late, a, b) * jnp.exp(-column(first, tr))
    return body


def silu_parts(p):
    sig = sigmoid(p)
    h = p * sig
    return h, sig + h * (1.0 - sig)


def backward(slots, layers, steps, stages):
    def body(flags, *refs):
        mines, refs = refs[:PIECES], refs[PIECES:]
        others, refs = [refs[k * PIECES:(k + 1) * PIECES] for k in range(stages)], refs[stages * PIECES:]
        din, dout, cg, w, head, ls, z, *refs = refs
        pres, enc, (sample, g1, g2), refs = refs[:layers], refs[layers], refs[layers + 1:layers + 4], refs[layers + 4:]
        wthi, wtlo, hhi, hlo, pg, cbuf, wbuf, dzbuf, small, later, ibuf, obuf, isems, osems = refs
        width = pg.shape[1]
        top = (layers // 2) * width
        tail = top + width // 2
        per_rays = mines[0].shape[0] - 8

        def add_grad(l, g):
            ref = g1 if l >= layers // 2 else g2
            rows = slice((l % (layers // 2)) * width, (l % (layers // 2) + 1) * width)
            ref[rows, :] += g

        phase, i = pl.program_id(0), pl.program_id(1)
        tr = SUB // slots
        nsub = steps * STEP
        per = nsub // PIECES
        n = nsub * tr
        blk = STEP * SUB
        mask = ray_mask(tr, SUB, slots)
        sources = list(pres) + [enc]

        def copy_in(l, k):
            rows = pl.ds(k * blk, blk)
            return pltpu.make_async_copy(sources[l].at[rows], ibuf.at[l, rows], isems.at[l, k])

        def copy_out(k):
            rows = pl.ds(k * blk, blk)
            return pltpu.make_async_copy(obuf.at[rows], sample.at[rows], osems.at[k])

        def rows_of(s):
            return pl.ds(i * blk + s * SUB, SUB)

        @pl.when((phase == 0) & (i == 0))
        def _():
            for k in range(steps):
                copy_in(layers - 1, k).start()
            for k in range(steps):
                for l in list(reversed(range(layers - 1))) + [layers]:
                    copy_in(l, k).start()
            px, sx = [], []
            for s in range(nsub):
                q, t = s // per, s % per
                at = slice(per_rays + t, per_rays + t + 1)
                rc = slice(t * tr, (t + 1) * tr)
                a, mt = mines[q][rc, :], mines[q][at, :]
                sf, off = jnp.zeros(a.shape, F32), jnp.zeros(mt.shape, F32)
                for k in range(stages):
                    late = flags[k] == 1
                    b, to = others[k][q][rc, :], others[k][q][at, :]
                    e = jnp.exp(-column(jnp.where(late, to, mt)[:, :tr], tr))
                    sf = jnp.where(late, sf * e, sf + b * e)
                    off = off + jnp.where(late, to, 0.0)
                    a, mt = jnp.where(late, b, a) + jnp.where(late, a, b) * e, mt + to
                px.append(a)
                sx.append(sf)
                offc = column(off[:, :tr], tr)
                later[s:s + 1, :] = jnp.sum(jnp.where(mask, offc, 0.0), axis=0, keepdims=True)
            px = split(jnp.concatenate(px, axis=0))
            small[...] = jnp.zeros(small.shape, F32)
            nc = cg.shape[0]
            small[:nc, :n] = cg[...]
            small[8:8 + nc, :dout.shape[1]] = dout[...]
            cg_t, dout_t = small[:8, :n], small[8:16, :dout.shape[1]]
            di = split(din[...])
            act, slope = silu_parts(dot3(px, di, NN))
            g1[...] = jnp.zeros(g1.shape, F32)
            g2[...] = jnp.zeros(g2.shape, F32)
            g1[tail + 8:tail + 16, :] = stacked(split(cg_t), split(act), NN)
            up = lax.dot_general(cg_t, dout_t, (TN, ((), ())), precision=HIGH, preferred_element_type=F32)
            dpre = split(up * slope)
            gin = dot3(px, dpre, TN)
            g1[top:tail, :] = gin[:width // 2]
            g2[top:tail, :] = gin[width // 2:]
            g = dot3(dpre, di, NT)
            pg[...] = g
            for s in range(nsub):
                rc = slice(s * tr, (s + 1) * tr)
                lc = jnp.sum(sx[s] * g[rc, :], axis=1, keepdims=True)
                later[8 + s:9 + s, :] = jnp.sum(jnp.where(mask, lc, 0.0), axis=0, keepdims=True)
            for l in range(layers):
                hi, lo = split(w[0, l].T)
                wthi[l] = hi
                wtlo[l] = lo

        @pl.when(phase == 0)
        def _():
            copy_in(layers - 1, i).wait()
            for s in range(STEP):
                sub = i * STEP + s
                p = ibuf[layers - 1, rows_of(s), :]
                h4 = split(p * sigmoid(p))
                hhi[sub] = h4[0]
                hlo[sub] = h4[1]
                g = pg[pl.ds(sub * tr, tr), :]
                c = stacked(split(g), h4, NT)
                cbuf[pl.ds(sub, 1), :] = jnp.sum(jnp.where(mask, c, 0.0), axis=0, keepdims=True)

        @pl.when((phase == 0) & (i == steps - 1))
        def _():
            slot = slot_of(z.shape, slots)
            zz, sp, c = z[...], ls[...], cbuf[...]
            tau = sp * softplus(zz)
            incl = scan_slots(tau, slots)
            trans = jnp.exp(-(later[:nsub, :] + (incl - tau)))
            weight = trans * one_minus_exp(tau)
            rest = scan_slots(weight * c, slots, reverse=True)
            after = later[8:8 + nsub, :] + jnp.where(slot + 1 < slots, pltpu.roll(rest, SUB - 1, 1), 0.0)
            dz = sp * jax.nn.sigmoid(zz) * (trans * jnp.exp(-tau) * c - after)
            wbuf[...] = weight
            dzbuf[...] = dz
            dh, dl = split(dz)
            acc = jnp.zeros((nsub, width), F32)
            row = lax.broadcasted_iota(jnp.int32, dz.shape, 0)
            for s in range(nsub):
                d = tuple(jnp.where(row == s, x.astype(F32), 0.0).astype(BF16) for x in (dh, dl))
                acc = acc + stacked(d, (hhi[s], hlo[s]), NN)
            g1[tail:tail + 1, :] = jnp.sum(acc, axis=0, keepdims=True)

        @pl.when(phase == 1)
        def _():
            for l in list(range(layers - 1)) + [layers]:
                copy_in(l, i).wait()
            first = lax.broadcasted_iota(jnp.int32, (16, SUB), 0) == 0
            backs, slopes = [], []
            for s in range(STEP):
                sub = i * STEP + s
                g = pg[pl.ds(sub * tr, tr), :]
                a = jnp.concatenate([
                    jnp.where(mask, jnp.broadcast_to(wbuf[pl.ds(sub, 1), :], (tr, SUB)), 0.0),
                    jnp.where(first, jnp.broadcast_to(dzbuf[pl.ds(sub, 1), :], (16, SUB)), 0.0)], axis=0)
                b = jnp.concatenate([g, jnp.broadcast_to(head[...], (16, g.shape[1]))], axis=0)
                ah, al = split(a)
                bh, bl = split(b)
                backs.append(dot1(jnp.concatenate([ah, al, ah], axis=0), jnp.concatenate([bh, bh, bl], axis=0), TN))
                slopes.append(silu_parts(ibuf[layers - 1, rows_of(s), :])[1])
            for l in reversed(range(layers)):
                for s in range(STEP):
                    dp = split(backs[s] * slopes[s])
                    if l:
                        h, slopes[s] = silu_parts(ibuf[l - 1, rows_of(s), :])
                    else:
                        h = ibuf[layers, rows_of(s), :]
                    backs[s] = dot3(dp, (wthi[l], wtlo[l]), NN)
                    if l == 0:
                        obuf[rows_of(s), :] = backs[s]
                    if l == 0 and s == STEP - 1:
                        copy_out(i).start()
                    add_grad(l, dot3(split(h), dp, TN))

        @pl.when((phase == 1) & (i == steps - 1))
        def _():
            for k in range(steps):
                copy_out(k).wait()
    return body


def finish(layers, width, colors):
    def body(flag, x1, got1, x2, got2, lg, hg, gin, gout):
        upper = flag[0] == 1
        half = layers // 2
        top, tail = half * width, half * width + width // 2

        def rows(piece, a, b):
            x, got = piece
            m = x.shape[0]
            parts = []
            if a < m:
                cut = slice(a, min(b, m))
                parts.append(jnp.where(upper, got[cut, :], x[cut, :]))
            if b > m:
                cut = slice(max(a, m) - m, b - m)
                parts.append(jnp.where(upper, x[cut, :], got[cut, :]))
            return parts[0] if len(parts) == 1 else jnp.concatenate(parts, axis=0)

        for l in range(layers):
            piece = (x1, got1) if l >= half else (x2, got2)
            lg[0, l] = rows(piece, (l % half) * width, (l % half + 1) * width)
        gin[:width // 2, :] = rows((x1, got1), top, tail)
        gin[width // 2:, :] = rows((x2, got2), top, tail)
        end = rows((x1, got1), tail, tail + 16)
        hg[...] = end[:1]
        gout[...] = end[8:8 + colors]
    return body


def pinned(x):
    return pltpu.with_memory_space_constraint(x, pltpu.HBM)


def full(shape):
    return pl.BlockSpec(shape, lambda *_: (0,) * len(shape))


def call(body, grid, ins, outs, scratch=(), vmem=8 << 20):
    return pl.pallas_call(
        body,
        grid=grid,
        in_specs=list(ins),
        out_specs=[s for s, _ in outs],
        out_shape=[sh for _, sh in outs],
        scratch_shapes=list(scratch),
        compiler_params=pltpu.CompilerParams(vmem_limit_bytes=vmem),
    )


def arr(*shape):
    return jax.ShapeDtypeStruct(shape, F32)


def swap(x, axis, bit):
    return lax.ppermute(x, axis, [(i, i ^ bit) for i in range(lax.axis_size(axis))])


def bits_of(axis):
    n = lax.axis_size(axis)
    return [1 << k for k in range(n.bit_length() - 1)]


def all_reduce(pieces, axis):
    me = lax.axis_index(axis)
    bits = bits_of(axis)
    pieces = list(pieces)
    plans = []
    for p in range(len(pieces)):
        order = bits if p == 0 else bits[:1] + bits[:0:-1]
        plans.append([(b, True) for b in order] + [(b, False) for b in reversed(order)])
    for turn in range(len(plans[0]) + SKEW * (len(pieces) - 1)):
        for p in reversed(range(len(pieces))):
            stages = plans[p]
            if not 0 <= turn - SKEW * p < len(stages):
                continue
            bit, halving = stages[turn - SKEW * p]
            upper = (me // bit) % 2
            x = pieces[p]
            if halving:
                half = x.shape[0] // 2
                keep = lax.dynamic_slice_in_dim(x, upper * half, half)
                send = lax.dynamic_slice_in_dim(x, (1 - upper) * half, half)
                pieces[p] = keep + swap(send, axis, bit)
            else:
                got = swap(x, axis, bit)
                if turn - SKEW * p == len(stages) - 1:
                    pieces[p] = (x, got)
                    continue
                pieces[p] = jnp.where(upper == 1, jnp.concatenate([got, x]), jnp.concatenate([x, got]))
    return pieces


def local(encodings, spacing, counts, cell_weights, density_head, decoder_in, decoder_out, color_grad):
    rays, slots, width = encodings.shape
    layers = cell_weights.shape[1]
    total_rows = rays * slots
    tr = SUB // slots
    nsub = total_rows // SUB
    blk = STEP * SUB
    steps = total_rows // blk
    rows = pinned(encodings.reshape(total_rows, width))
    weights = pinned(cell_weights)
    tile = pl.BlockSpec((blk, width), lambda i: (i, 0))
    wspec = full(cell_weights.shape)
    hspec = full((1, width))
    lane = full((nsub, SUB))
    prays = rays // PIECES
    ext = (prays + 8, width)
    hbm = pl.BlockSpec(memory_space=pl.ANY)
    *pres, z, ls = call(
        forward(slots, layers, steps), (steps,),
        [tile, wspec, hspec, full((slots, rays)), full((1, rays))],
        [(hbm, pltpu.HBM((total_rows, width), F32))] * layers
        + [(full(ext), arr(*ext))] * PIECES + [(lane, arr(nsub, SUB)), (lane, arr(nsub, SUB))],
        [pltpu.VMEM((layers, width, width), BF16)] * 2 + [pltpu.VMEM((nsub, SUB, width), BF16)] * 2
        + [pltpu.VMEM((layers, total_rows, width), F32), pltpu.SemaphoreType.DMA((layers, steps))],
        vmem=VMEM_F,
    )(rows, weights, pinned(density_head), pinned(spacing.T), pinned(counts.T))
    pres, totals = pres[:layers], pres[layers:]

    me = lax.axis_index("cell")
    smem = pl.BlockSpec(memory_space=pltpu.SMEM)
    bits = bits_of("cell")
    flags = jnp.stack([(me // bit) % 2 for bit in bits]).astype(jnp.int32)
    mines, others = list(totals), []
    for k, bit in enumerate(bits):
        others.append([swap(t, "cell", bit) for t in totals])
        if bit != bits[-1]:
            totals = [
                call(combine(k, tr), (1,), [smem, full(ext), full(ext)], [(full(ext), arr(*ext))])(flags, t, o)[0]
                for t, o in zip(totals, others[-1])]

    colors = color_grad.shape[1]
    sq = (width, width)

    def once(shape):
        return pl.BlockSpec(shape, lambda p, i: (0,) * len(shape))

    gshape = (layers, width, width)
    top = (layers // 2) * width + width // 2
    shape1, shape2 = (top + 64, width), (top, width)
    sample, g1, g2 = call(
        backward(slots, layers, steps, len(bits)), (2, steps),
        [smem] + [once(ext)] * (PIECES * (1 + len(bits)))
        + [once(sq), once((colors, width)), once((colors, rays)), once(cell_weights.shape), once((1, width)),
           once((nsub, SUB)), once((nsub, SUB))] + [hbm] * (layers + 1),
        [(hbm, pltpu.HBM((total_rows, width), F32)), (once(shape1), arr(*shape1)), (once(shape2), arr(*shape2))],
        [pltpu.VMEM(gshape, BF16)] * 2 + [pltpu.VMEM((nsub, SUB, width), BF16)] * 2
        + [pltpu.VMEM((rays, width), F32)] + [pltpu.VMEM((nsub, SUB), F32)] * 3
        + [pltpu.VMEM((16, max(rays, width)), F32), pltpu.VMEM((16, SUB), F32)]
        + [pltpu.VMEM((layers + 1, total_rows, width), F32), pltpu.VMEM((total_rows, width), F32)]
        + [pltpu.SemaphoreType.DMA((layers + 1, steps)), pltpu.SemaphoreType.DMA((steps,))],
        vmem=VMEM_B,
    )(flags, *mines, *[o for group in others for o in group], decoder_in, decoder_out.T, color_grad.T, weights,
      density_head, ls, z, *pres, rows)

    pieces = all_reduce([g1, g2], "rays")
    flag = (lax.axis_index("rays") % 2).astype(jnp.int32).reshape(1)
    h1, h2 = (top + 64) // 2, top // 2
    layer_grads, head_grads, din_grad, dout_grad = call(
        finish(layers, width, colors), (1,),
        [smem, full((h1, width)), full((h1, width)), full((h2, width)), full((h2, width))],
        [(full(cell_weights.shape), arr(*cell_weights.shape)), (full((1, width)), arr(1, width)), (full(sq), arr(*sq)),
         (full((colors, width)), arr(colors, width))], vmem=16 << 20,
    )(flag, *pieces[0], *pieces[1])
    return layer_grads, head_grads, din_grad, dout_grad.T, sample.reshape(rays, slots, width)


def solution(mesh):
    in_specs = (
        P("rays", "cell", None),
        P("rays", "cell"),
        P("rays", "cell"),
        P("cell", None, None, None),
        P("cell", None),
        P(),
        P(),
        P("rays", None),
    )
    out_specs = (P("cell", None, None, None), P("cell", None), P(), P(), P("rays", "cell", None))
    return jax.shard_map(local, mesh=mesh, in_specs=in_specs, out_specs=out_specs, check_vma=False)
```
